8 devices in a mesh: member: 2 (over z, y), lat: 4 (over x, core).
Axes of the slice: x: 2, y: 2, z: 1, core: 2. Of those that a mesh axis runs over, the one named last changes fastest.
Arguments:
- field_in: float32 [24, 128, 128, 256], P('member', None, 'lat'), parts along dimension 0
- grad_out: float32 [24, 128, 128, 256], P('member', None, 'lat'), parts along dimension 0
- p_fwd: float32 [128, 128, 128], replicated
- p_inv: float32 [128, 128, 128], replicated
- w_mix: float32 [128, 128, 128, 2], replicated
Outputs:
- output 1: float32 [24, 128, 128, 256], P('member', None, 'lat'), parts along dimension 0
- output 2: float32 [256, 128, 128, 2], P('member'), parts along dimension 0
There are 2 independent parts. The reference program is written for one: setup_inputs(seed, part) draws one part's arguments, and reference() takes and returns one part's arrays. A program takes and returns all parts, laid end to end along the dimension named above; an argument that names none is the same for every part.
All inputs are finite; a program needn't handle non-finite values.
Results may differ from the reference program's by a relative error of at most 0.00656286.
Values are sent between devices in bfloat16 or wider.
A program may use at most 1 GiB of HBM per device.

```python
import math
import jax
import jax.numpy as jnp
from jax import lax

BATCH = 12
CHANNELS = 128
NLAT = 128

NLON = 2 * NLAT


def setup_inputs(seed: int = 0, part: int = 0) -> dict:
    part_key = jax.random.fold_in(jax.random.key(seed), part)
    key_field, key_grad = jax.random.split(part_key, 2)
    key_fwd, key_inv, key_mix = jax.random.split(jax.random.key(seed + 1), 3)
    field_in = jax.random.normal(key_field, (BATCH, CHANNELS, NLAT, NLON), jnp.float32)
    grad_out = jax.random.normal(key_grad, (BATCH, CHANNELS, NLAT, NLON), jnp.float32)
    wave_num = jnp.arange(NLAT)[:, None, None]
    degree = jnp.arange(NLAT)[None, :, None]
    lower_tri = (degree >= wave_num).astype(jnp.float32)
    fwd_scale = lower_tri / math.sqrt(NLAT)
    inv_scale = lower_tri / jnp.sqrt((NLAT - wave_num).astype(jnp.float32))
    p_fwd = jax.random.normal(key_fwd, (NLAT, NLAT, NLAT), jnp.float32) * fwd_scale
    p_inv = jax.random.normal(key_inv, (NLAT, NLAT, NLAT), jnp.float32) * inv_scale
    w_mix = jax.random.normal(key_mix, (NLAT, CHANNELS, CHANNELS, 2), jnp.float32) / math.sqrt(2 * CHANNELS)
    return {'field_in': field_in, 'grad_out': grad_out, 'p_fwd': p_fwd, 'p_inv': p_inv, 'w_mix': w_mix}


def to_bf16(values):
    return values.astype(jnp.bfloat16).astype(jnp.float32)


def gelu_grad(values):
    cumulative = 0.5 * (1.0 + lax.erf(values * math.sqrt(0.5)))
    density = jnp.exp(-0.5 * values * values) / math.sqrt(2.0 * math.pi)
    return cumulative + values * density


def mix_matrix(w_mix):
    w_real = w_mix[..., 0]
    w_imag = w_mix[..., 1]
    upper_half = jnp.stack([w_real, -w_imag], axis=-1)
    lower_half = jnp.stack([w_imag, w_real], axis=-1)
    return jnp.stack([upper_half, lower_half], axis=2)


def analysis(values, mode_gains):
    spectrum = jnp.fft.rfft(values, axis=-1)[..., :NLAT] * mode_gains
    return jnp.stack([spectrum.real, spectrum.imag], axis=-2)


def synthesis(spec_pair, mode_gains):
    complex_spec = lax.complex(spec_pair[..., 0, :], spec_pair[..., 1, :]) * mode_gains
    padded = jnp.pad(complex_spec, [(0, 0)] * (complex_spec.ndim - 1) + [(0, NLON // 2 + 1 - NLAT)])
    return jnp.fft.irfft(padded, n=NLON, axis=-1)


def reference(field_in, grad_out, p_fwd, p_inv, w_mix):
    root_lon = math.sqrt(NLON)
    is_mean = jnp.arange(NLAT) == 0
    pw_half = to_bf16(p_fwd)
    pi_half = to_bf16(p_inv)
    w_big = to_bf16(mix_matrix(w_mix))
    four_lat = to_bf16(analysis(field_in, 1.0 / root_lon))
    coeffs = to_bf16(jnp.einsum('mlt,bctrm->bclrm', pw_half, four_lat))
    mixed_coef = to_bf16(jnp.einsum('losir,bilrm->bolsm', w_big, coeffs))
    back_lat = to_bf16(jnp.einsum('mlt,bclrm->bctrm', pi_half, mixed_coef))
    hidden = synthesis(back_lat, root_lon)
    grad_hidden = grad_out * gelu_grad(hidden)
    grad_back = to_bf16(analysis(grad_hidden, jnp.where(is_mean, 1.0, 2.0) / root_lon))
    grad_mixed = to_bf16(jnp.einsum('mlt,bctrm->bclrm', pi_half, grad_back))
    grad_big = jnp.einsum('bolsm,bilrm->losir', grad_mixed, coeffs)
    grad_coef = to_bf16(jnp.einsum('losir,bolsm->bilrm', w_big, grad_mixed))
    grad_four = to_bf16(jnp.einsum('mlt,bclrm->bctrm', pw_half, grad_coef))
    grad_field = grad_out + synthesis(grad_four, jnp.where(is_mean, 1.0, 0.5) * root_lon)
    grad_wmix = jnp.stack([grad_big[:, :, 0, :, 0] + grad_big[:, :, 1, :, 1], grad_big[:, :, 1, :, 0] - grad_big[:, :, 0, :, 1]], axis=-1)
    return grad_field, grad_wmix
```

```python
import functools
import math
import jax
import jax.numpy as jnp
import numpy as np
from jax import lax
from jax.experimental import pallas as pl
from jax.experimental.pallas import tpu as pltpu
from jax.sharding import PartitionSpec as P

BF16 = jnp.bfloat16
F32 = jnp.float32
LANES = 128
PAD = 8
VMEM_LIMIT = 60 * 1024 * 1024
NN = (((1,), (0,)), ((), ()))
NT = (((1,), (1,)), ((), ()))
TN = (((0,), (0,)), ((), ()))


def gelu_grad(values):
    cumulative = 0.5 * (1.0 + lax.erf(values * math.sqrt(0.5)))
    density = jnp.exp(-0.5 * values * values) * (1.0 / math.sqrt(2.0 * math.pi))
    return cumulative + values * density


def split(values):
    high = values.astype(BF16)
    low = (values - high.astype(F32)).astype(BF16)
    return high, low


def dot(lhs, rhs, dims):
    return lax.dot_general(lhs, rhs, dims, preferred_element_type=F32)


def fourier_rows(lon_count, mode_count, doubled):
    modes = np.arange(mode_count)[:, None]
    angle = 2.0 * np.pi * ((modes * np.arange(lon_count)[None, :]) % lon_count) / lon_count
    gain = np.where(modes == 0, 1.0, 2.0 if doubled else 1.0) / math.sqrt(lon_count)
    rows = np.concatenate([gain * np.cos(angle), -gain * np.sin(angle)], axis=0).astype(np.float32)
    high = rows.astype(BF16)
    low = (rows - high.astype(np.float32)).astype(BF16)
    return jnp.asarray(high), jnp.asarray(low)


def params():
    return pltpu.CompilerParams(vmem_limit_bytes=VMEM_LIMIT, dimension_semantics=("arbitrary",))


def cost(micros, bytes_accessed):
    return pl.CostEstimate(flops=int(micros * 1e6 * 200), bytes_accessed=int(bytes_accessed), transcendentals=0)


def load_rows(ref, pitch, rows_out, rows_in, source):
    def body(step, carry):
        for sub in range(8):
            row = step * 8 + sub
            ref[pl.ds(pl.multiple_of(row * pitch, 8), rows_in), :] = source(row)
        return carry
    lax.fori_loop(0, rows_out // 8, body, 0)


def analysis_tail(spec, half_refs, pitch, lat):
    for part in range(2):
        half_refs[part][pl.ds(pl.multiple_of(lat * pitch, 8), LANES), :] = spec[part * LANES:(part + 1) * LANES, :]


def emit_spectrum(out_ref, half_refs, pitch, dest_count, m_local, lat_local):
    def body(m_loc, carry):
        for dest in range(dest_count):
            for part in range(2):
                rows = half_refs[part][pl.ds(m_loc * dest_count + dest, lat_local, stride=pitch), :]
                out_ref[dest, 0, m_loc, :, part * LANES:(part + 1) * LANES] = rows.astype(BF16)
        return carry
    lax.fori_loop(0, m_local, body, 0, unroll=2)


def copy_field(field_ref, refs, pitch, lat_local):
    for half in range(2):
        load_rows(refs[half], pitch, LANES, lat_local,
                  lambda c, half=half: field_ref[0, c, :, half * LANES:(half + 1) * LANES])


def copy_spectrum(spec_ref, refs, pitch, dest_count, m_local, lat_local):
    def body(m_loc, carry):
        for src in range(dest_count):
            for part in range(2):
                refs[part][pl.ds(pl.multiple_of((m_loc * dest_count + src) * pitch, 8), lat_local), :] = (
                    spec_ref[src, 0, m_loc, :, part * LANES:(part + 1) * LANES].astype(F32))
        return carry
    lax.fori_loop(0, m_local, body, 0, unroll=2)


def analysis_kernel(field_ref, high_ref, low_ref, out_ref, f0, f1, s0, s1):
    dest_count, _, m_local, lat_local, _ = out_ref.shape
    pitch_t, pitch_m = lat_local + PAD, LANES + PAD
    copy_field(field_ref, (f0, f1), pitch_t, lat_local)

    def body(lat, carry):
        rows = jnp.concatenate([f0[pl.ds(lat, LANES, stride=pitch_t), :], f1[pl.ds(lat, LANES, stride=pitch_t), :]], axis=1)
        x_high, x_low = split(rows)
        spec = dot(high_ref[...], x_high, NT) + dot(low_ref[...], x_high, NT) + dot(high_ref[...], x_low, NT)
        analysis_tail(spec, (s0, s1), pitch_m, lat)
        return carry
    lax.fori_loop(0, lat_local, body, 0, unroll=2)
    emit_spectrum(out_ref, (s0, s1), pitch_m, dest_count, m_local, lat_local)


def middle_kernel(spec_ref, grad_ref, high_ref, low_ref, out_ref, g0, g1, f0, f1, s0, s1):
    dest_count, _, m_local, lat_local, _ = out_ref.shape
    pitch_t, pitch_m = lat_local + PAD, LANES + PAD
    copy_spectrum(spec_ref, (g0, g1), pitch_t, dest_count, m_local, lat_local)
    copy_field(grad_ref, (f0, f1), pitch_t, lat_local)

    def body(lat, carry):
        coef = jnp.concatenate([g0[pl.ds(lat, LANES, stride=pitch_t), :], g1[pl.ds(lat, LANES, stride=pitch_t), :]], axis=0).astype(BF16)
        hidden = dot(coef, high_ref[...], TN) + dot(coef, low_ref[...], TN)
        grad = jnp.concatenate([f0[pl.ds(lat, LANES, stride=pitch_t), :], f1[pl.ds(lat, LANES, stride=pitch_t), :]], axis=1)
        x_high, x_low = split(grad * gelu_grad(hidden))
        spec = dot(high_ref[...], x_high, NT) + dot(low_ref[...], x_high, NT) + dot(high_ref[...], x_low, NT)
        analysis_tail(spec, (s0, s1), pitch_m, lat)
        return carry
    lax.fori_loop(0, lat_local, body, 0, unroll=2)
    emit_spectrum(out_ref, (s0, s1), pitch_m, dest_count, m_local, lat_local)


def final_kernel(first, *refs):
    if first:
        spec_ref, grad_ref, high_ref, low_ref, out_ref, g0, g1, f0, f1 = refs
    else:
        spec_ref, grad_ref, high_ref, low_ref, _, out_ref, g0, g1, f0, f1 = refs
    dest_count, _, m_local, lat_local, _ = spec_ref.shape
    pitch_t = lat_local + PAD
    copy_spectrum(spec_ref, (g0, g1), pitch_t, dest_count, m_local, lat_local)

    def body(lat, carry):
        coef = jnp.concatenate([g0[pl.ds(lat, LANES, stride=pitch_t), :], g1[pl.ds(lat, LANES, stride=pitch_t), :]], axis=0).astype(BF16)
        wave = dot(coef, high_ref[...], TN) + dot(coef, low_ref[...], TN)
        f0[pl.ds(lat, LANES, stride=pitch_t), :] = wave[:, :LANES]
        f1[pl.ds(lat, LANES, stride=pitch_t), :] = wave[:, LANES:]
        return carry
    lax.fori_loop(0, lat_local, body, 0, unroll=2)

    def emit(step, carry):
        for sub in range(8):
            chan = step * 8 + sub
            for half, ref in enumerate((f0, f1)):
                cols = slice(half * LANES, (half + 1) * LANES)
                out_ref[0, chan, :, cols] = grad_ref[0, chan, :, cols] + ref[pl.ds(pl.multiple_of(chan * pitch_t, 8), lat_local), :]
        return carry
    lax.fori_loop(0, LANES // 8, emit, 0)


def legendre_kernel(spec_ref, poly_ref, out_ref, s0, s1):
    src_count, _, m_local, lat_local, _ = spec_ref.shape
    pitch = LANES + PAD

    def body(m_loc, carry):
        rows = jnp.concatenate([spec_ref[src, 0, m_loc] for src in range(src_count)], axis=0)
        coef = dot(poly_ref[m_loc], rows, NN)
        for part, ref in enumerate((s0, s1)):
            ref[pl.ds(pl.multiple_of(m_loc * pitch, 8), LANES), :] = coef[:, part * LANES:(part + 1) * LANES]
        return carry
    lax.fori_loop(0, m_local, body, 0, unroll=4)

    def emit(degree, carry):
        for part, ref in enumerate((s0, s1)):
            out_ref[degree, :, part * LANES:(part + 1) * LANES] = ref[pl.ds(degree, m_local, stride=pitch), :].astype(BF16)
        return carry
    lax.fori_loop(0, LANES, emit, 0, unroll=8)


def inverse_kernel(coef_ref, poly_ref, out_ref, s0, s1):
    dest_count, _, m_local, lat_local, _ = out_ref.shape
    pitch = m_local + PAD

    def fill(degree, carry):
        for part, ref in enumerate((s0, s1)):
            ref[pl.ds(pl.multiple_of(degree * pitch, 8), m_local), :] = coef_ref[degree, :, part * LANES:(part + 1) * LANES].astype(F32)
        return carry
    lax.fori_loop(0, LANES, fill, 0, unroll=8)

    def body(m_loc, carry):
        rows = jnp.concatenate([ref[pl.ds(m_loc, LANES, stride=pitch), :] for ref in (s0, s1)], axis=1).astype(BF16)
        back = dot(poly_ref[m_loc], rows, NN).astype(BF16)
        for dest in range(dest_count):
            out_ref[dest, 0, m_loc] = back[dest * lat_local:(dest + 1) * lat_local, :]
        return carry
    lax.fori_loop(0, m_local, body, 0, unroll=4)


def mix_kernel(coef_ref, mix_ref, out_ref):
    for k in range(coef_ref.shape[0]):
        out_ref[k] = dot(coef_ref[k], mix_ref[k], NT).astype(BF16)


def mixback_kernel(first, *refs):
    if first:
        dq_ref, coef_ref, mix_ref, out_ref, gw_ref = refs
    else:
        dq_ref, coef_ref, mix_ref, prev_ref, out_ref, gw_ref = refs
    for k in range(coef_ref.shape[0]):
        dq = dq_ref[k]
        coef = coef_ref[k]
        out_ref[k] = dot(dq, mix_ref[k], NN).astype(BF16)
        lhs = jnp.concatenate([dq[:, :LANES], dq[:, LANES:]], axis=0)
        rhs = jnp.concatenate([
            jnp.concatenate([coef[:, :LANES], -coef[:, LANES:]], axis=1),
            jnp.concatenate([coef[:, LANES:], coef[:, :LANES]], axis=1)], axis=0)
        grad = dot(lhs, rhs, TN)
        for part in range(2):
            piece = grad[:, part * LANES:(part + 1) * LANES]
            gw_ref[k, part] = piece if first else prev_ref[k, part] + piece


def solution(mesh):
    lat_size = mesh.shape['lat']
    field_spec = P('member', None, 'lat', None)
    chunk_count = 4

    def local_step(field_loc, grad_loc, p_fwd, p_inv, w_mix):
        batch, channels, lat_local, lon_count = field_loc.shape
        lat_count = p_fwd.shape[-1]
        m_local = lat_count // lat_size
        chunk = batch // chunk_count
        own = lax.axis_index('lat')
        d_high, d_low = fourier_rows(lon_count, lat_count, False)
        c_high, c_low = fourier_rows(lon_count, lat_count, True)

        def own_modes(poly):
            grouped = poly.reshape(m_local, lat_size, lat_count, lat_count)
            return lax.dynamic_index_in_dim(grouped, own, 1, keepdims=False).astype(BF16)

        pw_own, pi_own = own_modes(p_fwd), own_modes(p_inv)
        pw_back, pi_back = jnp.swapaxes(pw_own, 1, 2), jnp.swapaxes(pi_own, 1, 2)
        w_real, w_imag = w_mix[..., 0].astype(BF16), w_mix[..., 1].astype(BF16)
        w_big = jnp.concatenate([jnp.concatenate([w_real, -w_imag], axis=2), jnp.concatenate([w_imag, w_real], axis=2)], axis=1)

        spec_shape = jax.ShapeDtypeStruct((lat_size, chunk, m_local, lat_local, 2 * channels), BF16)
        coef_shape = jax.ShapeDtypeStruct((lat_count, chunk * m_local, 2 * channels), BF16)
        gw_shape = jax.ShapeDtypeStruct((lat_count, 2, channels, channels), F32)
        spec_block = pl.BlockSpec((lat_size, 1, m_local, lat_local, 2 * channels), lambda b: (0, b, 0, 0, 0))
        coef_block = pl.BlockSpec((lat_count, m_local, 2 * channels), lambda b: (0, b, 0))
        four_block = pl.BlockSpec((2 * lat_count, lon_count), lambda b: (0, 0))
        poly_block = pl.BlockSpec((m_local, lat_count, lat_count), lambda b: (0, 0, 0))

        def field_block(k):
            return pl.BlockSpec((1, channels, lat_local, lon_count), lambda b: (b + k * chunk, 0, 0, 0))

        fields = [pltpu.VMEM((channels * (lat_local + PAD), LANES), F32)] * 2
        spectra = [pltpu.VMEM((lat_count * (lat_local + PAD), LANES), F32)] * 2
        latspec = [pltpu.VMEM((lat_local * (lat_count + PAD), LANES), F32)] * 2
        legscr = [pltpu.VMEM((m_local * (lat_count + PAD), LANES), F32)] * 2
        invscr = [pltpu.VMEM((lat_count * (m_local + PAD), LANES), F32)] * 2
        mb = 1e6

        def analyse(k):
            return pl.pallas_call(analysis_kernel, grid=(chunk,), name="analyse", out_shape=spec_shape,
                                  in_specs=[field_block(k), four_block, four_block], out_specs=spec_block,
                                  scratch_shapes=fields + latspec, compiler_params=params(), cost_estimate=cost(20, 20 * mb))(field_loc, d_high, d_low)

        def middle(k, spec):
            return pl.pallas_call(middle_kernel, grid=(chunk,), name="middle", out_shape=spec_shape,
                                  in_specs=[spec_block, field_block(k), four_block, four_block], out_specs=spec_block,
                                  scratch_shapes=spectra + fields + latspec, compiler_params=params(), cost_estimate=cost(45, 26 * mb))(spec, grad_loc, c_high, c_low)

        def finish(k, spec, prev):
            first = prev is None
            extra = [] if first else [pl.BlockSpec(memory_space=pl.ANY)]
            args = [spec, grad_loc, d_high, d_low] + ([] if first else [prev])
            return pl.pallas_call(functools.partial(final_kernel, first), grid=(chunk,), name="finish",
                                  out_shape=jax.ShapeDtypeStruct(field_loc.shape, F32),
                                  in_specs=[spec_block, field_block(k), four_block, four_block] + extra, out_specs=field_block(k),
                                  input_output_aliases={} if first else {4: 0},
                                  scratch_shapes=spectra + fields, compiler_params=params(), cost_estimate=cost(20, 32 * mb))(*args)

        def legendre(spec, poly):
            return pl.pallas_call(legendre_kernel, grid=(chunk,), name="legendre", out_shape=coef_shape,
                                  in_specs=[spec_block, poly_block], out_specs=coef_block, scratch_shapes=legscr,
                                  compiler_params=params(), cost_estimate=cost(10, 14 * mb))(spec, poly)

        def inverse(coef, poly):
            return pl.pallas_call(inverse_kernel, grid=(chunk,), name="inverse", out_shape=spec_shape,
                                  in_specs=[coef_block, poly_block], out_specs=spec_block, scratch_shapes=invscr,
                                  compiler_params=params(), cost_estimate=cost(10, 14 * mb))(coef, poly)

        step_l = 8
        row_block = pl.BlockSpec((step_l, chunk * m_local, 2 * channels), lambda l: (l, 0, 0))
        mix_block = pl.BlockSpec((step_l, 2 * channels, 2 * channels), lambda l: (l, 0, 0))
        gw_block = pl.BlockSpec((step_l, 2, channels, channels), lambda l: (l, 0, 0, 0))

        def mix(coef):
            return pl.pallas_call(mix_kernel, grid=(lat_count // step_l,), name="mix", out_shape=coef_shape,
                                  in_specs=[row_block, mix_block], out_specs=row_block,
                                  compiler_params=params(), cost_estimate=cost(12, 30 * mb))(coef, w_big)

        def mixback(dq, coef, prev):
            first = prev is None
            args = [dq, coef, w_big] + ([] if first else [prev])
            return pl.pallas_call(functools.partial(mixback_kernel, first), grid=(lat_count // step_l,), name="mixback",
                                  out_shape=[coef_shape, gw_shape],
                                  in_specs=[row_block, row_block, mix_block] + ([] if first else [gw_block]), out_specs=[row_block, gw_block],
                                  input_output_aliases={} if first else {3: 1},
                                  compiler_params=params(), cost_estimate=cost(25, 70 * mb))(*args)

        def exchange(spec):
            return lax.all_to_all(spec, 'lat', 0, 0, tiled=True)

        def swap(values, bit):
            return lax.ppermute(values, 'lat', [(d, d ^ bit) for d in range(lat_size)])

        chunks = range(chunk_count)
        spec = [exchange(analyse(k)) for k in chunks]
        coef = [legendre(spec[k], pw_own) for k in chunks]
        spec = [exchange(inverse(mix(coef[k]), pi_back)) for k in chunks]
        spec = [exchange(middle(k, spec[k])) for k in chunks]
        gw = None
        out = []
        for k in chunks:
            dq = legendre(spec[k], pi_own)
            da, gw = mixback(dq, coef[k], gw)
            out.append(exchange(inverse(da, pw_back)))

        core, chip = own % 2, own // 2
        halves = gw.reshape(2, lat_count // 2, 2, channels, channels)
        half = lax.dynamic_index_in_dim(halves, core, 0, keepdims=False) + swap(lax.dynamic_index_in_dim(halves, 1 - core, 0, keepdims=False), 1)
        quarters = half.reshape(2, lat_count // 4, 2, channels, channels)
        quarter = lax.dynamic_index_in_dim(quarters, chip, 0, keepdims=False) + swap(lax.dynamic_index_in_dim(quarters, 1 - chip, 0, keepdims=False), 2)
        other = swap(quarter, 2)
        half = jnp.where(chip == 0, jnp.stack([quarter, other]), jnp.stack([other, quarter]))
        far = swap(half, 1)
        full = jnp.where(core == 0, jnp.stack([half, far]), jnp.stack([far, half])).reshape(lat_count, 2, channels, channels)
        grad_wmix = jnp.transpose(full, (0, 2, 3, 1))

        grad_field = None
        for k in chunks:
            grad_field = finish(k, out[k], grad_field)
        return grad_field, grad_wmix

    return jax.shard_map(local_step, mesh=mesh, in_specs=(field_spec, field_spec, P(), P(), P()), out_specs=(field_spec, P('member', None, None, None)), check_vma=False)
```
